32 devices in a mesh: param: 8 (over z, y), freq: 4 (over x, core).
Axes of the slice: x: 2, y: 2, z: 4, core: 2. Of those that a mesh axis runs over, the one named last changes fastest.
Arguments:
- kernel_hat: bfloat16 [2, 16, 600, 8192], P(None, 'freq', None, 'param'), may hold values from -0.25 to 0.25
- prior_gain: float32 [16, 8192], P('freq', 'param'), may hold values from 0.00045776367 to 0.018310547, as said below
- noise_var: float32 [600], replicated, may hold values from 0.5 to 2
- observed: float32 [8, 16, 600], P('param', 'freq'), may hold values from -6 to 6
Outputs:
- solution: float32 [8, 16, 600], P('param', 'freq')
- residual: float32 [8, 16, 600], P('param', 'freq')
The draws below stay inside these ranges and needn't reach their ends.
Inputs may be any that keep to these rules, and one draw needn't show every extreme that they name: `prior_gain`: prior variances are positive.
All inputs are finite; a program needn't handle non-finite values.
Results may differ from the reference program's by a relative error of at most 0.0085.
Values may be sent and summed in bfloat16 or wider, within the bound.
A program may use at most 64 MiB of HBM per device.

```python
import math
import jax
import jax.numpy as jnp
from jax import lax

NS = 600
NT = 16
P_DEV = 1024
ITERS = 2
NP = 8192
R = 8


def draw_prior_gain(key, part):
    blocks = NP // P_DEV
    first_key, second_key = jax.random.split(jax.random.fold_in(key, 11))
    spread_base = jnp.exp(jax.random.uniform(first_key, (NT, NP), jnp.float32, jnp.log(0.2), jnp.log(2.0)))
    ranking = jax.random.permutation(second_key, blocks)
    weighty = (ranking < 2).astype(jnp.float32)
    factor = 1.0 + weighty * (0.5 * blocks - 1.0)
    overall = 0.5 * NS / (NT * NP)
    return (spread_base * jnp.repeat(factor, P_DEV)[None, :] * overall).astype(jnp.float32)


def shard_levels(rng, dims, shards, smallest, largest):
    factor_of, own = 1.0, jax.random.fold_in(rng, 6)
    for axis_at, shards_of in shards:
        draws = jnp.exp(jax.random.uniform(jax.random.fold_in(own, axis_at), (shards_of,), jnp.float32, smallest / len(shards), largest / len(shards)))
        factor_of = factor_of * jnp.repeat(draws, dims[axis_at] // shards_of).reshape([-1 if axis == axis_at else 1 for axis in range(len(dims))])
    return factor_of


def noise(own_key, shape, deviation, reach, cuts=(), kind=jnp.bfloat16):
    factor_of = shard_levels(own_key, shape, cuts, -0.22, 0.18) if cuts else 1.0
    result = jax.random.normal(own_key, shape, jnp.float32) * deviation * factor_of
    return jnp.minimum(jnp.maximum(result, -reach), reach).astype(kind)


def setup_inputs(seed: int = 0) -> dict:
    streams_of = jax.random.split(jax.random.key(seed), 5)
    return {
        "kernel_hat": noise(streams_of[0], (2, NT, NS, NP), NS ** -0.5, 0.25, ((1, 4), (3, 8))),
        "prior_gain": draw_prior_gain(jax.random.fold_in(streams_of[4], 71), 0),
        "noise_var": jnp.clip(jnp.exp(jax.random.uniform(streams_of[2], (NS,), jnp.float32, math.log(0.5), math.log(2.0))), 0.5, 2.0),
        "observed": noise(streams_of[3], (R, NT, NS), 1.0, 6.0, ((0, 8), (1, 4)), jnp.float32),
    }


HIGHEST = lax.Precision.HIGHEST


def phase_tables(freq_first, freq_count, time_first, time_count, period):
    freq_ids = freq_first + lax.iota(jnp.int32, freq_count)
    time_ids = time_first + lax.iota(jnp.int32, time_count)
    phase_int = (freq_ids[:, None] * time_ids[None, :]) % period
    phase = phase_int.astype(jnp.float32) * (2.0 * math.pi / period)
    return jnp.cos(phase), jnp.sin(phase)


def apply_hessian(fields, kernel_hat, prior_gain, noise_var):
    period = 2 * NT - 1
    cosines, sines = phase_tables(0, NT, 0, NT, period)
    spec_real = jnp.einsum("kt,rts->krs", cosines, fields, precision=HIGHEST).astype(jnp.bfloat16)
    spec_imag = (-jnp.einsum("kt,rts->krs", sines, fields, precision=HIGHEST)).astype(jnp.bfloat16)

    def one_slot(slot_id):
        real_part = kernel_hat[0, slot_id]
        imag_part = kernel_hat[1, slot_id]
        upper = spec_real[slot_id]
        lower = spec_imag[slot_id]
        coef_real = jnp.dot(upper, real_part, preferred_element_type=jnp.float32) + jnp.dot(lower, imag_part, preferred_element_type=jnp.float32)
        coef_imag = jnp.dot(lower, real_part, preferred_element_type=jnp.float32) - jnp.dot(upper, imag_part, preferred_element_type=jnp.float32)
        slot_gain = prior_gain[slot_id]
        coef_real = (coef_real * slot_gain[None, :]).astype(jnp.bfloat16)
        coef_imag = (coef_imag * slot_gain[None, :]).astype(jnp.bfloat16)
        image_real = jnp.dot(coef_real, real_part.T, preferred_element_type=jnp.float32) - jnp.dot(coef_imag, imag_part.T, preferred_element_type=jnp.float32)
        image_imag = jnp.dot(coef_imag, real_part.T, preferred_element_type=jnp.float32) + jnp.dot(coef_real, imag_part.T, preferred_element_type=jnp.float32)
        return image_real, image_imag

    image_real, image_imag = lax.map(one_slot, jnp.arange(NT, dtype=jnp.int32))
    inverse = jnp.einsum("krs,kt->rts", image_real, cosines, precision=HIGHEST) - jnp.einsum("krs,kt->rts", image_imag, sines, precision=HIGHEST)
    return noise_var[None, None, :] * fields + inverse


def reference(kernel_hat, prior_gain, noise_var, observed):
    solution = jnp.zeros_like(observed)
    residual = observed
    direction = observed
    norm_now = jnp.sum(residual * residual, axis=(1, 2))
    for sweep in range(ITERS):
        applied = apply_hessian(direction, kernel_hat, prior_gain, noise_var)
        step_len = norm_now / jnp.sum(direction * applied, axis=(1, 2))
        solution = solution + step_len[:, None, None] * direction
        residual = residual - step_len[:, None, None] * applied
        norm_next = jnp.sum(residual * residual, axis=(1, 2))
        direction = residual + (norm_next / norm_now)[:, None, None] * direction
        norm_now = norm_next
    return solution, residual
```

```python
import functools
import math

import jax
import jax.numpy as jnp
import numpy as np
from jax import lax
from jax.experimental import pallas as pl
from jax.experimental.pallas import tpu as pltpu
from jax.sharding import PartitionSpec as P

ITERS = 2
LANES = 128
F32 = jnp.float32
BF16 = jnp.bfloat16
HIGHEST = lax.Precision.HIGHEST


def phase_tables(freqs, times):
    period = 2 * times - 1
    ids = np.arange(freqs)[:, None] * np.arange(times)[None, :] % period
    phase = ids.astype(np.float32) * np.float32(2.0 * math.pi / period)
    return np.cos(phase).astype(np.float32), np.sin(phase).astype(np.float32)


def kernel(
    n_param,
    n_freq,
    obs_ref,
    kernel_ref,
    gain_ref,
    noise_ref,
    fwd_ref,
    inv_ref,
    sol_ref,
    res_ref,
    k_buf,
    obs_buf,
    sp_send,
    sp_buf,
    sp_wide,
    img_send,
    img_buf,
    row_send,
    row_buf,
    k_sem,
    obs_sems,
    sp_sems,
    img_sems,
    row_sems,
):
    _, slots, sensors, _ = kernel_ref.shape
    padded = k_buf.shape[2]
    tiles = padded // LANES
    comps = 2 * slots
    me_p = lax.axis_index("param")
    me_f = lax.axis_index("freq")

    loads = [
        pltpu.make_async_copy(
            kernel_ref.at[:, k], k_buf.at[:, k, pl.ds(0, sensors)], k_sem.at[k]
        )
        for k in range(slots)
    ]
    for load in loads:
        load.start()
    k_buf[:, :, sensors:, :] = jnp.zeros(
        (2, slots, padded - sensors, k_buf.shape[3]), BF16
    )

    barrier = pltpu.get_barrier_semaphore()
    for d in range(1, n_freq):
        pl.semaphore_signal(
            barrier, inc=1, device_id={"freq": lax.rem(me_f + d, n_freq)}
        )
    for d in range(1, n_param):
        pl.semaphore_signal(
            barrier, inc=1, device_id={"param": lax.rem(me_p + d, n_param)}
        )
    pl.semaphore_wait(barrier, n_freq + n_param - 2)

    def exchange(axis, me, n, source, target, sems):
        sent = []
        for d in range(1, n):
            peer = lax.rem(me + d, n)
            copy = pltpu.make_async_remote_copy(
                src_ref=source(peer),
                dst_ref=target.at[me],
                send_sem=sems.at[0, peer],
                recv_sem=sems.at[1, me],
                device_id={axis: peer},
            )
            copy.start()
            sent.append(copy)

        def arrive():
            for d in range(1, n):
                peer = lax.rem(me + n - d, n)
                pltpu.make_async_remote_copy(
                    src_ref=source(peer),
                    dst_ref=target.at[peer],
                    send_sem=sems.at[0, peer],
                    recv_sem=sems.at[1, peer],
                    device_id={axis: peer},
                ).wait_recv()

        def left():
            for copy in sent:
                copy.wait_send()

        return arrive, left

    pending = []
    block = obs_ref.shape[0]
    obs_buf[me_f] = obs_ref[...]
    arrive, left = exchange(
        "freq", me_f, n_freq, lambda peer: obs_ref, obs_buf, obs_sems
    )
    pending.append(left)
    arrive()
    tail = jnp.zeros((block * n_freq, padded - sensors), F32)
    field = jnp.concatenate([obs_buf[j] for j in range(n_freq)], axis=0)
    field = jnp.concatenate([field, tail], axis=1)
    noise = jnp.concatenate([noise_ref[...], tail[:1]], axis=1)

    fwd = fwd_ref[me_f]
    inv = inv_ref[...]
    solution = jnp.zeros_like(field)
    residual = field
    direction = field
    norm_now = jnp.sum(residual * residual, keepdims=True)
    for sweep in range(ITERS):
        spectra = jnp.dot(fwd, direction, precision=HIGHEST, preferred_element_type=F32)
        spectra = spectra.astype(BF16)
        sp_send[sweep] = spectra
        arrive, left = exchange(
            "param",
            me_p,
            n_param,
            lambda peer: sp_send.at[sweep],
            sp_buf.at[sweep],
            sp_sems.at[sweep],
        )
        pending.append(left)
        sp_buf[sweep, me_p] = spectra
        arrive()
        for r in range(n_param):
            wide = sp_buf[sweep, r].astype(F32)
            for l in range(tiles):
                sp_wide[l, r * comps : (r + 1) * comps, :] = wide[
                    :, l * LANES : (l + 1) * LANES
                ]

        def rows_of(comp):
            return jnp.concatenate(
                [
                    sp_wide[l, pl.ds(comp, n_param, stride=comps), :]
                    for l in range(tiles)
                ],
                axis=1,
            )

        for k in range(slots):
            if sweep == 0:
                loads[k].wait()
            upper, lower = rows_of(k), rows_of(slots + k)
            first = jnp.concatenate([upper, lower], axis=0).astype(BF16)
            second = jnp.concatenate([lower, -upper], axis=0).astype(BF16)
            coef = jnp.dot(
                first, k_buf[0, k], preferred_element_type=F32
            ) + jnp.dot(second, k_buf[1, k], preferred_element_type=F32)
            coef = coef * gain_ref[k : k + 1, :]
            turned = jnp.concatenate([-coef[n_param:], coef[:n_param]], axis=0)
            contract = (((1,), (1,)), ((), ()))
            image = lax.dot_general(
                coef.astype(BF16), k_buf[0, k], contract, preferred_element_type=F32
            ) + lax.dot_general(
                turned.astype(BF16), k_buf[1, k], contract, preferred_element_type=F32
            )
            for c in range(2):
                for l in range(tiles):
                    img_send[
                        sweep, l, pl.ds(c * slots + k, n_param, stride=comps), :
                    ] = image[
                        c * n_param : (c + 1) * n_param, l * LANES : (l + 1) * LANES
                    ]

        def part(peer):
            start = pl.multiple_of(peer * comps, comps)
            return img_send.at[sweep, :, pl.ds(start, comps), :]

        arrive, left = exchange(
            "param", me_p, n_param, part, img_buf.at[sweep], img_sems.at[sweep]
        )
        pending.append(left)
        img_buf[sweep, me_p] = img_send[
            sweep, :, pl.ds(pl.multiple_of(me_p * comps, comps), comps), :
        ]
        arrive()
        total = img_buf[sweep, 0]
        for r in range(1, n_param):
            total = total + img_buf[sweep, r]
        row_send[sweep] = total
        arrive, left = exchange(
            "freq",
            me_f,
            n_freq,
            lambda peer: row_send.at[sweep],
            row_buf.at[sweep],
            row_sems.at[sweep],
        )
        pending.append(left)
        row_buf[sweep, me_f] = total
        arrive()
        image = jnp.concatenate(
            [
                jnp.concatenate([row_buf[sweep, j, l] for l in range(tiles)], axis=1)
                for j in range(n_freq)
            ],
            axis=0,
        )
        inverse = jnp.dot(inv, image, precision=HIGHEST, preferred_element_type=F32)
        applied = noise * direction + inverse
        step_len = norm_now / jnp.sum(direction * applied, keepdims=True)
        solution = solution + step_len * direction
        residual = residual - step_len * applied
        if sweep + 1 < ITERS:
            norm_next = jnp.sum(residual * residual, keepdims=True)
            direction = residual + (norm_next / norm_now) * direction
            norm_now = norm_next

    for out_ref, value in ((sol_ref, solution), (res_ref, residual)):
        own = value[:block]
        for j in range(1, n_freq):
            own = jnp.where(me_f == j, value[j * block : (j + 1) * block], own)
        out_ref[...] = own[:, :sensors]
    for left in pending:
        left()


def solution(mesh):
    n_param, n_freq = mesh.shape["param"], mesh.shape["freq"]

    def local(kernel_hat, prior_gain, noise_var, observed):
        _, slots, sensors, params = kernel_hat.shape
        rows, block, _ = observed.shape
        assert rows == 1
        times = block * n_freq
        padded = -(-sensors // LANES) * LANES
        tiles = padded // LANES
        comps = 2 * slots
        cos, sin = phase_tables(slots * n_freq, times)
        pieces = np.stack([cos, -sin]).reshape(2, n_freq, slots, times)
        forward = pieces.transpose(1, 0, 2, 3).reshape(n_freq, comps, times)
        inverse = forward.reshape(n_freq * comps, times).T.copy()
        vmem = pl.BlockSpec(memory_space=pltpu.VMEM)
        out = jax.ShapeDtypeStruct((block, sensors), F32)
        dma = pltpu.SemaphoreType.DMA
        results = pl.pallas_call(
            functools.partial(kernel, n_param, n_freq),
            out_shape=(out, out),
            in_specs=[vmem, pl.BlockSpec(memory_space=pl.ANY)] + [vmem] * 4,
            out_specs=(vmem, vmem),
            scratch_shapes=[
                pltpu.VMEM((2, slots, padded, params), BF16),
                pltpu.VMEM((n_freq, block, sensors), F32),
                pltpu.VMEM((ITERS, comps, padded), BF16),
                pltpu.VMEM((ITERS, n_param, comps, padded), BF16),
                pltpu.VMEM((tiles, n_param * comps, LANES), F32),
                pltpu.VMEM((ITERS, tiles, n_param * comps, LANES), F32),
                pltpu.VMEM((ITERS, n_param, tiles, comps, LANES), F32),
                pltpu.VMEM((ITERS, tiles, comps, LANES), F32),
                pltpu.VMEM((ITERS, n_freq, tiles, comps, LANES), F32),
                dma((slots,)),
                dma((2, n_freq)),
                dma((ITERS, 2, n_param)),
                dma((ITERS, 2, n_param)),
                dma((ITERS, 2, n_freq)),
            ],
            compiler_params=pltpu.CompilerParams(
                collective_id=0,
                has_side_effects=True,
                vmem_limit_bytes=48 * 1024 * 1024,
            ),
        )(
            observed.reshape(block, sensors),
            kernel_hat,
            prior_gain,
            noise_var.reshape(1, sensors),
            jnp.asarray(forward),
            jnp.asarray(inverse),
        )
        return tuple(value.reshape(observed.shape) for value in results)

    return jax.shard_map(
        local,
        mesh=mesh,
        in_specs=(
            P(None, "freq", None, "param"),
            P("freq", "param"),
            P(),
            P("param", "freq", None),
        ),
        out_specs=(P("param", "freq", None), P("param", "freq", None)),
        check_vma=False,
    )
```

```python
import functools
import math

import jax
import jax.numpy as jnp
import numpy as np
from jax import lax
from jax.experimental import pallas as pl
from jax.experimental.pallas import tpu as pltpu
from jax.sharding import PartitionSpec as P

ITERS = 2
LANES = 128
CHUNK = 5
F32 = jnp.float32
BF16 = jnp.bfloat16
HIGHEST = lax.Precision.HIGHEST


def phase_tables(freqs, times):
    period = 2 * times - 1
    ids = np.arange(freqs)[:, None] * np.arange(times)[None, :] % period
    phase = ids.astype(np.float32) * np.float32(2.0 * math.pi / period)
    return np.cos(phase).astype(np.float32), np.sin(phase).astype(np.float32)


def sensor_chunks(padded):
    tiles = padded // LANES
    return [(t, min(CHUNK, tiles - t)) for t in range(0, tiles, CHUNK)]


def kernel(
    n_param,
    n_freq,
    obs_ref,
    kernel_ref,
    gain_ref,
    noise_ref,
    fwd_ref,
    inv_ref,
    sol_ref,
    res_ref,
    k_buf,
    obs_buf,
    gain_buf,
    noise_buf,
    fwd_buf,
    inv_buf,
    fwd_wide,
    inv_wide,
    sp_send,
    sp_buf,
    sp_wide,
    img_send,
    img_buf,
    row_send,
    row_buf,
    k_sem,
    small_sem,
    obs_sems,
    sp_sems,
    img_sems,
    row_sems,
):
    _, slots, sensors, _ = kernel_ref.shape
    padded = k_buf.shape[2]
    tiles = padded // LANES
    chunks = sensor_chunks(padded)
    comps = 2 * slots
    me_p = lax.axis_index("param")
    me_f = lax.axis_index("freq")

    barrier = pltpu.get_barrier_semaphore()
    for d in range(1, n_freq):
        pl.semaphore_signal(
            barrier, inc=1, device_id={"freq": lax.rem(me_f + d, n_freq)}
        )
    for d in range(1, n_param):
        pl.semaphore_signal(
            barrier, inc=1, device_id={"param": lax.rem(me_p + d, n_param)}
        )
    small = [
        pltpu.make_async_copy(obs_ref.at[0], obs_buf.at[me_f], small_sem.at[0]),
        pltpu.make_async_copy(gain_ref, gain_buf, small_sem.at[1]),
        pltpu.make_async_copy(noise_ref, noise_buf, small_sem.at[2]),
        pltpu.make_async_copy(fwd_ref.at[me_f], fwd_buf, small_sem.at[3]),
        pltpu.make_async_copy(inv_ref, inv_buf, small_sem.at[4]),
    ]
    loads = []
    for i, (first, count) in enumerate(chunks):
        rows = pl.ds(first * LANES, min(count * LANES, sensors - first * LANES))
        loads.append(
            pltpu.make_async_copy(
                kernel_ref.at[:, :, rows], k_buf.at[:, :, rows], k_sem.at[i]
            )
        )
    for load in small + loads:
        load.start()
    k_buf[:, :, sensors:, :] = jnp.zeros(
        (2, slots, padded - sensors, k_buf.shape[3]), BF16
    )

    pl.semaphore_wait(barrier, n_freq + n_param - 2)

    def exchange(axis, me, n, source, target, sems):
        sent = []
        for d in range(1, n):
            peer = lax.rem(me + d, n)
            copy = pltpu.make_async_remote_copy(
                src_ref=source(peer),
                dst_ref=target(me),
                send_sem=sems.at[0, peer],
                recv_sem=sems.at[1, me],
                device_id={axis: peer},
            )
            copy.start()
            sent.append(copy)

        inbound = []
        for d in range(1, n):
            peer = lax.rem(me + n - d, n)
            inbound.append(
                pltpu.make_async_remote_copy(
                    src_ref=source(peer),
                    dst_ref=target(peer),
                    send_sem=sems.at[0, peer],
                    recv_sem=sems.at[1, peer],
                    device_id={axis: peer},
                )
            )

        def arrive():
            for copy in inbound:
                copy.wait_recv()

        def left():
            for copy in sent:
                copy.wait_send()

        return arrive, left

    pending = []
    block = obs_ref.shape[1]
    small[0].wait()
    arrive, left = exchange(
        "freq",
        me_f,
        n_freq,
        lambda peer: obs_buf.at[me_f],
        lambda slot: obs_buf.at[slot],
        obs_sems,
    )
    pending.append(left)
    for copy in small[1:]:
        copy.wait()
    for table, wide in ((fwd_buf, fwd_wide), (inv_buf, inv_wide)):
        held = table[...]
        for m in range(wide.shape[0]):
            wide[m] = jnp.broadcast_to(held[:, m : m + 1], wide.shape[1:])

    def weighted(wide, rows):
        sums = [wide[m] * row for m, row in enumerate(rows)]
        while len(sums) > 1:
            sums = [sum(sums[m : m + 2]) for m in range(0, len(sums), 2)]
        return sums[0]

    arrive()
    tail = jnp.zeros((block * n_freq, padded - sensors), F32)
    field = jnp.concatenate([obs_buf[j] for j in range(n_freq)], axis=0)
    field = jnp.concatenate([field, tail], axis=1)
    noise = jnp.concatenate([noise_buf[...].reshape(1, sensors), tail[:1]], axis=1)

    solution = jnp.zeros_like(field)
    residual = field
    direction = field
    norm_now = jnp.sum(residual * residual, keepdims=True)
    for sweep in range(ITERS):
        waits = []
        for i, (head, count) in enumerate(chunks):
            lanes = pl.ds(head * LANES, count * LANES)
            stretch = direction[:, head * LANES : (head + count) * LANES]
            spectra = jnp.concatenate(
                [
                    weighted(
                        fwd_wide,
                        [
                            stretch[t : t + 1, l * LANES : (l + 1) * LANES]
                            for t in range(block * n_freq)
                        ],
                    )
                    for l in range(count)
                ],
                axis=1,
            ).astype(BF16)
            sp_send[sweep, :, lanes] = spectra
            arrive, left = exchange(
                "param",
                me_p,
                n_param,
                lambda peer: sp_send.at[sweep, :, lanes],
                lambda slot: sp_buf.at[sweep, slot, :, lanes],
                sp_sems.at[sweep, i],
            )
            sp_buf[sweep, me_p, :, lanes] = spectra
            waits.append(arrive)
            pending.append(left)

        coefs = [0.0] * slots
        for i, (head, count) in enumerate(chunks):
            lanes = pl.ds(head * LANES, count * LANES)
            waits[i]()
            if sweep == 0:
                loads[i].wait()
            for r in range(n_param):
                wide = sp_buf[sweep, r, :, lanes].astype(F32)
                for l in range(count):
                    sp_wide[head + l, r * comps : (r + 1) * comps, :] = wide[
                        :, l * LANES : (l + 1) * LANES
                    ]

            def rows_of(comp):
                return jnp.concatenate(
                    [
                        sp_wide[head + l, pl.ds(comp, n_param, stride=comps), :]
                        for l in range(count)
                    ],
                    axis=1,
                )

            for k in range(slots):
                upper, lower = rows_of(k), rows_of(slots + k)
                ahead = jnp.concatenate([upper, lower], axis=0).astype(BF16)
                turned = jnp.concatenate([lower, -upper], axis=0).astype(BF16)
                coefs[k] = (
                    coefs[k]
                    + jnp.dot(ahead, k_buf[0, k, lanes], preferred_element_type=F32)
                    + jnp.dot(turned, k_buf[1, k, lanes], preferred_element_type=F32)
                )

        pairs = []
        for k in range(slots):
            coef = coefs[k] * gain_buf[k : k + 1, :]
            turned = jnp.concatenate([-coef[n_param:], coef[:n_param]], axis=0)
            pairs.append((coef.astype(BF16), turned.astype(BF16)))
        contract = (((1,), (1,)), ((), ()))
        waits = []
        for i, (head, count) in enumerate(chunks):
            lanes = pl.ds(head * LANES, count * LANES)
            span = pl.ds(head, count)
            for k in range(slots):
                image = lax.dot_general(
                    pairs[k][0], k_buf[0, k, lanes], contract, preferred_element_type=F32
                ) + lax.dot_general(
                    pairs[k][1], k_buf[1, k, lanes], contract, preferred_element_type=F32
                )
                for c in range(2):
                    for l in range(count):
                        img_send[
                            sweep,
                            head + l,
                            pl.ds(c * slots + k, n_param, stride=comps),
                            :,
                        ] = image[
                            c * n_param : (c + 1) * n_param,
                            l * LANES : (l + 1) * LANES,
                        ]

            def part(peer):
                start = pl.multiple_of(peer * comps, comps)
                return img_send.at[sweep, span, pl.ds(start, comps), :]

            arrive, left = exchange(
                "param",
                me_p,
                n_param,
                part,
                lambda slot: img_buf.at[sweep, slot, span],
                img_sems.at[sweep, i],
            )
            waits.append(arrive)
            pending.append(left)

        late = []
        own = pl.ds(pl.multiple_of(me_p * comps, comps), comps)
        for i, (head, count) in enumerate(chunks):
            span = pl.ds(head, count)
            img_buf[sweep, me_p, span] = img_send[sweep, span, own, :]
            waits[i]()
            total = img_buf[sweep, 0, span]
            for r in range(1, n_param):
                total = total + img_buf[sweep, r, span]
            row_send[sweep, span] = total
            arrive, left = exchange(
                "freq",
                me_f,
                n_freq,
                lambda peer: row_send.at[sweep, span],
                lambda slot: row_buf.at[sweep, slot, span],
                row_sems.at[sweep, i],
            )
            row_buf[sweep, me_f, span] = total
            late.append(arrive)
            pending.append(left)

        inverse = []
        for i, (head, count) in enumerate(chunks):
            late[i]()
            for l in range(head, head + count):
                inverse.append(
                    weighted(
                        inv_wide,
                        [
                            row_buf[sweep, j, l, c : c + 1, :]
                            for j in range(n_freq)
                            for c in range(comps)
                        ],
                    )
                )
        applied = noise * direction + jnp.concatenate(inverse, axis=1)
        step_len = norm_now / jnp.sum(direction * applied, keepdims=True)
        solution = solution + step_len * direction
        residual = residual - step_len * applied
        if sweep + 1 < ITERS:
            norm_next = jnp.sum(residual * residual, keepdims=True)
            direction = residual + (norm_next / norm_now) * direction
            norm_now = norm_next

    for out_ref, value in ((sol_ref, solution), (res_ref, residual)):
        own = value[:block]
        for j in range(1, n_freq):
            own = jnp.where(me_f == j, value[j * block : (j + 1) * block], own)
        out_ref[...] = own[:, :sensors]
    for left in pending:
        left()


def solution(mesh):
    n_param, n_freq = mesh.shape["param"], mesh.shape["freq"]

    def local(kernel_hat, prior_gain, noise_var, observed):
        _, slots, sensors, params = kernel_hat.shape
        rows, block, _ = observed.shape
        assert rows == 1
        times = block * n_freq
        padded = -(-sensors // LANES) * LANES
        tiles = padded // LANES
        parts = len(sensor_chunks(padded))
        comps = 2 * slots
        cos, sin = phase_tables(slots * n_freq, times)
        pieces = np.stack([cos, -sin]).reshape(2, n_freq, slots, times)
        forward = pieces.transpose(1, 0, 2, 3).reshape(n_freq, comps, times)
        inverse = forward.reshape(n_freq * comps, times).T.copy()
        vmem = pl.BlockSpec(memory_space=pltpu.VMEM)
        out = jax.ShapeDtypeStruct((block, sensors), F32)
        dma = pltpu.SemaphoreType.DMA
        results = pl.pallas_call(
            functools.partial(kernel, n_param, n_freq),
            out_shape=(out, out),
            in_specs=[pl.BlockSpec(memory_space=pltpu.HBM)] * 6,
            out_specs=(vmem, vmem),
            scratch_shapes=[
                pltpu.VMEM((2, slots, padded, params), BF16),
                pltpu.VMEM((n_freq, block, sensors), F32),
                pltpu.VMEM((slots, params), F32),
                pltpu.VMEM((sensors,), F32),
                pltpu.VMEM((comps, times), F32),
                pltpu.VMEM(inverse.shape, F32),
                pltpu.VMEM((times, comps, LANES), F32),
                pltpu.VMEM((comps * n_freq, times, LANES), F32),
                pltpu.VMEM((ITERS, comps, padded), BF16),
                pltpu.VMEM((ITERS, n_param, comps, padded), BF16),
                pltpu.VMEM((tiles, n_param * comps, LANES), F32),
                pltpu.VMEM((ITERS, tiles, n_param * comps, LANES), F32),
                pltpu.VMEM((ITERS, n_param, tiles, comps, LANES), F32),
                pltpu.VMEM((ITERS, tiles, comps, LANES), F32),
                pltpu.VMEM((ITERS, n_freq, tiles, comps, LANES), F32),
                dma((parts,)),
                dma((5,)),
                dma((2, n_freq)),
                dma((ITERS, parts, 2, n_param)),
                dma((ITERS, parts, 2, n_param)),
                dma((ITERS, parts, 2, n_freq)),
            ],
            compiler_params=pltpu.CompilerParams(
                collective_id=0,
                has_side_effects=True,
            ),
        )(
            observed,
            kernel_hat,
            prior_gain,
            noise_var,
            jnp.asarray(forward),
            jnp.asarray(inverse),
        )
        return tuple(value.reshape(observed.shape) for value in results)

    return jax.shard_map(
        local,
        mesh=mesh,
        in_specs=(
            P(None, "freq", None, "param"),
            P("freq", "param"),
            P(),
            P("param", "freq", None),
        ),
        out_specs=(P("param", "freq", None), P("param", "freq", None)),
        check_vma=False,
    )
```
